32 devices in a mesh: mrow: 2 (over y), pcol: 16 (over z, x, core).
Axes of the slice: x: 2, y: 2, z: 4, core: 2. Of those that a mesh axis runs over, the one named last changes fastest.
Arguments:
- snapshots: bfloat16 [7424, 4096], P('mrow', 'pcol'), may hold values from -16 to 16
- area_weight: float32 [4096], P('pcol'), may hold values from 0.2 to 1
Outputs:
- gram_tiles: float32 [2, 16, 1722368], P('mrow', 'pcol')
The draws below stay inside these ranges and needn't reach their ends.
All inputs are finite; a program needn't handle non-finite values.
Results may differ from the reference program's by a relative error of at most 0.0003.
Values may be sent and summed in bfloat16 or wider, within the bound.
A program may use at most 128 MiB of HBM per device.

```python
import math
import jax
import jax.numpy as jnp
from jax import lax

MEMBERS = 7424
POINTS = 4096
N_MROW = 2
N_PCOL = 16


def draw_snapshots(key, part):
    base = jax.random.fold_in(key, 11)
    keys = jax.random.split(base, 6)
    mode_count = 96
    climate = 2.0 * jax.random.normal(keys[0], (1, POINTS), jnp.float32)
    ranks = jnp.arange(1, mode_count + 1).astype(jnp.float32)
    coeff = jax.random.normal(keys[1], (MEMBERS, mode_count), jnp.float32) * (ranks ** (-0.5))[None, :]
    freq = jax.random.randint(keys[2], (mode_count, 1), 1, 33).astype(jnp.float32)
    phase = jax.random.uniform(keys[3], (mode_count, 1), jnp.float32, 0.0, 2.0 * math.pi)
    position = (jnp.arange(POINTS).astype(jnp.float32) / POINTS)[None, :]
    shapes = math.sqrt(2.0) * jnp.cos(2.0 * math.pi * freq * position + phase)
    rough = jax.random.uniform(keys[4], (1, POINTS), jnp.float32, 0.6, 1.4)
    total_var = jnp.sum(1.0 / ranks)
    signal = jnp.dot(coeff, shapes, precision=lax.Precision.HIGHEST) / jnp.sqrt(total_var) * rough
    noise = jax.random.normal(keys[5], (MEMBERS, POINTS), jnp.float32)
    field = signal + 0.2 * noise
    return jnp.clip(climate + field, -16.0, 16.0).astype(jnp.bfloat16)


def levels(own_key, shape, cuts, low, top_value):
    loudness = 1.0
    for dim, shards_of in cuts:
        draws = jax.random.uniform(jax.random.fold_in(jax.random.fold_in(own_key, 6), dim), (shards_of,), jnp.float32, low / len(cuts), top_value / len(cuts))
        loudness = loudness * jnp.repeat(jnp.exp(draws), shape[dim] // shards_of).reshape((-1,) + (1,) * (len(shape) - 1 - dim))
    return loudness


def setup_inputs(seed: int = 0) -> dict:
    key_list = jax.random.split(jax.random.key(seed), 3)
    snapshots = draw_snapshots(jax.random.fold_in(key_list[2], 71), 0)
    area_weight = jnp.clip(jnp.exp(math.log(1.0) - 1.609438 * jax.random.uniform(key_list[1], (POINTS,), jnp.float32) ** levels(key_list[1], (POINTS,), ((0, 16),), -0.2, 0.2)), 0.2, 1.0)
    return {"snapshots": snapshots, "area_weight": area_weight}


def reference(snapshots, area_weight):
    ens_mean = lax.optimization_barrier(jnp.sum(snapshots.astype(jnp.float32), axis=0)) / MEMBERS
    anomaly = ((snapshots.astype(jnp.float32) - ens_mean[None, :]) * jnp.sqrt(area_weight)[None, :]).astype(jnp.bfloat16)
    wide = anomaly.astype(jnp.float32)
    gram = jnp.dot(wide, wide.T, precision=lax.Precision.HIGHEST, preferred_element_type=jnp.float32)
    gram = gram / (MEMBERS - 1)
    blocks = gram.reshape(N_MROW, MEMBERS // N_MROW, N_PCOL, MEMBERS // N_PCOL)
    blocks = jnp.transpose(blocks, (0, 2, 1, 3))
    return blocks.reshape(N_MROW, N_PCOL, MEMBERS // N_MROW * (MEMBERS // N_PCOL))
```

```python
import functools

import jax
import jax.numpy as jnp
from jax import lax
from jax.experimental import pallas as pl
from jax.experimental.pallas import tpu as pltpu
from jax.sharding import PartitionSpec as P

MEMBERS = 7424
MESH = pl.DeviceIdType.MESH


def gather_gram(n_row, n_col, chunks, tile, a_ref, out_ref, full, cols, in_sem, recv, send, col_recv, col_send):
    rows, depth = a_ref.shape
    length = n_col // 4
    size = rows // chunks
    span = cols.shape[1]
    i = lax.axis_index("mrow")
    me = lax.axis_index("pcol")
    core = lax.rem(me, 2)
    side = lax.rem(me // 2, 2)
    line = me // 4
    ratio = n_col // n_row
    root = me // ratio
    offset = lax.rem(me, ratio) * tile
    aligned = pl.multiple_of(offset // 16 * 16, 16)
    my_chunk = aligned // size

    def index(where, which, own):
        return (where * 2 + which) * 2 + own

    up, down = index(line + 1, side, core), index(line - 1, side, core)
    across, sibling = index(line, 1 - side, core), index(line, side, 1 - core)
    has_up, has_down = line + 1 < length, line >= 1
    peers = [lax.rem(i + step, n_row) for step in range(1, n_row)]
    owns_cols = root == i

    barrier = pltpu.get_barrier_semaphore()

    def greet(row, col):
        pl.semaphore_signal(barrier, inc=1, device_id=(row, col), device_id_type=MESH)

    load = pltpu.make_async_copy(a_ref, full.at[me], in_sem)
    load.start()
    pl.when(has_up)(lambda: greet(i, up))
    pl.when(has_down)(lambda: greet(i, down))
    greet(i, across)
    greet(i, sibling)
    for peer in peers:
        greet(peer, me)
    out_ref[...] = jnp.zeros_like(out_ref)
    load.wait()
    pl.semaphore_wait(barrier, 2 + len(peers) + has_up.astype(jnp.int32) + has_down.astype(jnp.int32))

    def part(s, k):
        return full.at[s, pl.ds(pl.multiple_of(k * size, 16), size)]

    def copy(s, k, way, target):
        return pltpu.make_async_remote_copy(
            src_ref=part(s, k), dst_ref=part(s, k), send_sem=send.at[way, s], recv_sem=recv.at[s, k],
            device_id=(i, target), device_id_type=MESH,
        )

    def col_copy(s, n):
        return pltpu.make_async_remote_copy(
            src_ref=full.at[s, pl.ds(aligned, span)], dst_ref=cols.at[s], send_sem=col_send.at[n],
            recv_sem=col_recv.at[s], device_id=(peers[n], me), device_id_type=MESH,
        )

    def arrived(s, k):
        pltpu.make_async_copy(part(s, k), part(s, k), recv.at[s, k]).wait()

    def share(s, k):
        copy(s, k, 3, sibling).start()

    def to_peers(s, k):
        @pl.when(jnp.logical_and(owns_cols, k == my_chunk))
        def _():
            for n in range(len(peers)):
                col_copy(s, n).start()

    def go_up(s, k):
        pl.when(has_up)(lambda: copy(s, k, 0, up).start())

    def go_down(s, k):
        pl.when(has_down)(lambda: copy(s, k, 1, down).start())

    def own(k, _):
        copy(me, k, 2, across).start()
        go_up(me, k)
        go_down(me, k)
        share(me, k)
        to_peers(me, k)
        return 0

    lax.fori_loop(0, chunks, own, 0)
    arrived(across, 0)
    go_up(across, 0)
    go_down(across, 0)
    share(across, 0)
    to_peers(across, 0)

    def valid(sign, distance):
        place = line + sign * distance
        inside = jnp.logical_and(place >= 0, place < length)
        far = distance >= 1 if sign > 0 else distance >= 0
        return jnp.logical_and(inside, far)

    def step(d, _):
        def from_sibling(k):
            for sign in (-1, 1):
                for which, distance in ((side, d), (1 - side, d - 1)):
                    @pl.when(valid(sign, distance))
                    def _():
                        s = index(line + sign * distance, which, 1 - core)
                        arrived(s, k)
                        to_peers(s, k)

        def piece(k, _):
            for sign, forward in ((-1, go_up), (1, go_down)):
                @pl.when(valid(sign, d))
                def _():
                    s = index(line + sign * d, side, core)
                    arrived(s, k)
                    forward(s, k)
                    pl.when(k >= 1)(lambda: copy(s, k, 2, across).start())
                    share(s, k)
                    to_peers(s, k)

                    @pl.when(k == 0)
                    def _():
                        t = index(line + sign * d, 1 - side, core)
                        arrived(t, 0)
                        forward(t, 0)
                        share(t, 0)
                        to_peers(t, 0)

            for sign in (-1, 1):
                @pl.when(jnp.logical_and(valid(sign, d - 1), k >= 1))
                def _():
                    s = index(line + sign * (d - 1), 1 - side, core)
                    arrived(s, k)
                    share(s, k)
                    to_peers(s, k)

            pl.when(k >= 1)(lambda: from_sibling(k - 1))
            multiply(d - 1, k)
            return 0

        lax.fori_loop(0, chunks, piece, 0)
        from_sibling(chunks - 1)
        for sign in (-1, 1):
            for which, distance in ((side, d), (1 - side, d - 1)):
                for other in (core, 1 - core):
                    pl.when(valid(sign, distance))(
                        lambda: take_cols(index(line + sign * distance, which, other))
                    )
        return 0

    def take_cols(s):
        @pl.when(owns_cols)
        def _():
            cols[s] = full[s, pl.ds(aligned, span), :]

        @pl.when(jnp.logical_not(owns_cols))
        def _():
            pltpu.make_async_copy(cols.at[s], cols.at[s], col_recv.at[s]).wait()

    def multiply(d, k):
        row = pl.ds(pl.multiple_of(k * size, 16), size)

        def one(n, _):
            sign = 1 - 2 * (n // 4)
            cross = lax.rem(n // 2, 2)
            distance = d - cross
            place = line + sign * distance
            good = jnp.logical_and(place >= 0, place < length)
            good = jnp.logical_and(good, distance >= n // 4)
            good = jnp.logical_and(good, distance >= 0)

            @pl.when(good)
            def _():
                s = index(place, lax.rem(side + cross, 2), lax.rem(n, 2))
                right = cols[s]
                if span != tile:
                    right = jnp.where(offset == aligned, right[:tile], right[span - tile:])
                out_ref[row, :] += lax.dot_general(
                    full[s, row, :], right, (((1,), (1,)), ((), ())), preferred_element_type=jnp.float32
                )

            return 0

        lax.fori_loop(0, 8, one, 0)

    def ready_own(k, _):
        s = index(line, side, 1 - core)
        arrived(s, k)
        to_peers(s, k)
        return 0

    lax.fori_loop(0, chunks, ready_own, 0)
    take_cols(me)
    take_cols(sibling)
    lax.fori_loop(1, length + 1, step, 0)

    def last(k, _):
        multiply(length, k)
        return 0

    lax.fori_loop(0, chunks, last, 0)
    out_ref[...] = out_ref[...] / (MEMBERS - 1)

    def sent(s, way, first, count):
        ref = full.at[s, pl.ds(first * size, count * size)]
        pltpu.make_async_copy(ref, ref, send.at[way, s]).wait()

    def drain(place, _):
        straight, cross = index(place, side, core), index(place, 1 - side, core)
        sent(straight, 3, 0, chunks)
        sent(cross, 3, 0, chunks)
        pl.when(place == line)(lambda: sent(straight, 2, 0, chunks))
        pl.when(place != line)(lambda: sent(straight, 2, 1, chunks - 1))

        @pl.when(jnp.logical_and(has_up, place <= line))
        def _():
            sent(straight, 0, 0, chunks)
            sent(cross, 0, 0, 1)

        @pl.when(jnp.logical_and(has_down, place >= line))
        def _():
            sent(straight, 1, 0, chunks)
            sent(cross, 1, 0, 1)

        return 0

    lax.fori_loop(0, length, drain, 0)

    @pl.when(owns_cols)
    def _():
        for n in range(len(peers)):
            pltpu.make_async_copy(cols, cols, col_send.at[n]).wait()


def local(n_row, n_col, snapshots, area_weight):
    rows, depth = snapshots.shape
    tile = rows * n_row // n_col
    chunks = 8
    while rows % (16 * chunks):
        chunks //= 2
    span = tile + tile % 16
    local_sum = jnp.sum(snapshots.astype(jnp.float32), axis=0)
    ens_mean = lax.psum(local_sum, "mrow") / MEMBERS
    anomaly = (
        (snapshots.astype(jnp.float32) - ens_mean[None, :]) * jnp.sqrt(area_weight)[None, :]
    ).astype(jnp.bfloat16)
    gram = pl.pallas_call(
        functools.partial(gather_gram, n_row, n_col, chunks, tile),
        out_shape=jax.ShapeDtypeStruct((rows, tile), jnp.float32),
        in_specs=[pl.BlockSpec(memory_space=pl.ANY)],
        out_specs=pl.BlockSpec(memory_space=pltpu.VMEM),
        scratch_shapes=[
            pltpu.VMEM((n_col, rows, depth), jnp.bfloat16),
            pltpu.VMEM((n_col, span, depth), jnp.bfloat16),
            pltpu.SemaphoreType.DMA,
            pltpu.SemaphoreType.DMA((n_col, chunks)),
            pltpu.SemaphoreType.DMA((4, n_col)),
            pltpu.SemaphoreType.DMA((n_col,)),
            pltpu.SemaphoreType.DMA((max(n_row - 1, 1),)),
        ],
        compiler_params=pltpu.CompilerParams(
            collective_id=0, has_side_effects=True, vmem_limit_bytes=60 * 2**20
        ),
        name="gather_gram",
    )(anomaly)
    return gram.reshape(1, 1, rows * tile)


def solution(mesh):
    placed = (P("mrow", "pcol"), P("pcol"))
    return jax.shard_map(
        functools.partial(local, mesh.shape["mrow"], mesh.shape["pcol"]),
        mesh=mesh, in_specs=placed, out_specs=P("mrow", "pcol", None), check_vma=False,
    )
```

```python
import functools

import jax
import jax.numpy as jnp
from jax import lax
from jax.experimental import pallas as pl
from jax.experimental.pallas import tpu as pltpu
from jax.sharding import PartitionSpec as P

MEMBERS = 7424
MAX_CHUNKS = 32
MESH = pl.DeviceIdType.MESH


def gather_gram(
    n_row, n_col, chunks, early, pieces, tile, x_ref, weight_ref, out_ref, full, cols, sums, recv, send, col_recv, col_send,
    sum_recv, sum_send,
):
    rows, depth = x_ref.shape
    length = n_col // 4
    size = rows // chunks
    span = cols.shape[1]
    i = lax.axis_index("mrow")
    me = lax.axis_index("pcol")
    core = lax.rem(me, 2)
    side = lax.rem(me // 2, 2)
    line = me // 4
    ratio = n_col // n_row
    root = me // ratio
    offset = lax.rem(me, ratio) * tile
    aligned = pl.multiple_of(offset // 16 * 16, 16)
    my_chunk = (aligned + span - 1) // size
    stride = chunks // pieces

    def index(where, which, own):
        return (where * 2 + which) * 2 + own

    up, down = index(line + 1, side, core), index(line - 1, side, core)
    across, sibling = index(line, 1 - side, core), index(line, side, 1 - core)
    has_up, has_down = line + 1 < length, line >= 1
    peers = [lax.rem(i + step, n_row) for step in range(1, n_row)]
    owns_cols = root == i

    barrier = pltpu.get_barrier_semaphore()

    def greet(row, col):
        pl.semaphore_signal(barrier, inc=1, device_id=(row, col), device_id_type=MESH)

    pl.when(has_up)(lambda: greet(i, up))
    pl.when(has_down)(lambda: greet(i, down))
    greet(i, across)
    greet(i, sibling)
    for peer in peers:
        greet(peer, me)

    def add_up(k, total):
        block = x_ref[pl.ds(pl.multiple_of(k * size, 16), size), :].astype(jnp.float32)
        return total + jnp.sum(block.reshape(size // 8, 8, depth), axis=0)

    sums[i] = lax.fori_loop(0, chunks, add_up, jnp.zeros((8, depth), jnp.float32))
    pl.semaphore_wait(barrier, 2 + len(peers) + has_up.astype(jnp.int32) + has_down.astype(jnp.int32))

    def part(s, k):
        return full.at[s, pl.ds(pl.multiple_of(k * size, 16), size)]

    def copy(s, k, way, target):
        return pltpu.make_async_remote_copy(
            src_ref=part(s, k), dst_ref=part(s, k), send_sem=send.at[way, s], recv_sem=recv.at[s, k],
            device_id=(i, target), device_id_type=MESH,
        )

    def col_copy(s, n):
        return pltpu.make_async_remote_copy(
            src_ref=full.at[s, pl.ds(aligned, span)], dst_ref=cols.at[s], send_sem=col_send.at[n],
            recv_sem=col_recv.at[s], device_id=(peers[n], me), device_id_type=MESH,
        )

    def arrived(s, k):
        pltpu.make_async_copy(part(s, k), part(s, k), recv.at[s, k]).wait()

    def share(s, k):
        copy(s, k, 3, sibling).start()

    def to_peers(s, k):
        @pl.when(jnp.logical_and(owns_cols, k == my_chunk))
        def _():
            for n in range(len(peers)):
                col_copy(s, n).start()

    def go_up(s, k):
        pl.when(has_up)(lambda: copy(s, k, 0, up).start())

    def go_down(s, k):
        pl.when(has_down)(lambda: copy(s, k, 1, down).start())

    def sum_copy(n):
        return pltpu.make_async_remote_copy(
            src_ref=sums.at[i], dst_ref=sums.at[i], send_sem=sum_send.at[n], recv_sem=sum_recv.at[i],
            device_id=(peers[n], me), device_id_type=MESH,
        )

    for n in range(len(peers)):
        sum_copy(n).start()
    out_ref[...] = jnp.zeros_like(out_ref)
    for peer in peers:
        pltpu.make_async_copy(sums.at[peer], sums.at[peer], sum_recv.at[peer]).wait()
    mean = jnp.sum(jnp.sum(sums[...], axis=0), axis=0, keepdims=True) / MEMBERS
    root_weight = jnp.sqrt(weight_ref[...])

    def center(k):
        row = pl.ds(pl.multiple_of(k * size, 16), size)
        full[me, row, :] = ((x_ref[row, :].astype(jnp.float32) - mean) * root_weight).astype(jnp.bfloat16)

    def own(k, _):
        pl.when(k + 1 < chunks)(lambda: center(k + 1))
        copy(me, k, 2, across).start()
        go_up(me, k)
        go_down(me, k)
        share(me, k)
        to_peers(me, k)
        return 0

    center(0)
    lax.fori_loop(0, chunks, own, 0)

    def cross_first(k, _):
        arrived(across, k)
        go_up(across, k)
        go_down(across, k)
        share(across, k)
        to_peers(across, k)
        return 0

    lax.fori_loop(0, early, cross_first, 0)

    def valid(sign, distance):
        place = line + sign * distance
        inside = jnp.logical_and(place >= 0, place < length)
        far = distance >= 1 if sign > 0 else distance >= 0
        return jnp.logical_and(inside, far)

    def step(d, _):
        def from_sibling(k):
            for sign in (-1, 1):
                for which, distance in ((side, d), (1 - side, d - 1)):
                    @pl.when(valid(sign, distance))
                    def _():
                        s = index(line + sign * distance, which, 1 - core)
                        arrived(s, k)
                        to_peers(s, k)

        def piece(k, _):
            for sign, forward in ((-1, go_up), (1, go_down)):
                @pl.when(valid(sign, d))
                def _():
                    s = index(line + sign * d, side, core)
                    arrived(s, k)
                    forward(s, k)
                    pl.when(k >= early)(lambda: copy(s, k, 2, across).start())
                    share(s, k)
                    to_peers(s, k)

                    @pl.when(k < early)
                    def _():
                        t = index(line + sign * d, 1 - side, core)
                        arrived(t, k)
                        forward(t, k)
                        share(t, k)
                        to_peers(t, k)

            for sign in (-1, 1):
                @pl.when(jnp.logical_and(valid(sign, d - 1), k >= early))
                def _():
                    s = index(line + sign * (d - 1), 1 - side, core)
                    arrived(s, k)
                    share(s, k)
                    to_peers(s, k)

            pl.when(k >= 1)(lambda: from_sibling(k - 1))

            @pl.when(jnp.logical_and(lax.rem(k, stride) == stride - 1, k // stride < pieces))
            def _():
                multiply(d - 1, k // stride)

            return 0

        lax.fori_loop(0, chunks, piece, 0)
        from_sibling(chunks - 1)
        for sign in (-1, 1):
            for which, distance in ((side, d), (1 - side, d - 1)):
                for other in (core, 1 - core):
                    pl.when(valid(sign, distance))(
                        lambda: take_cols(index(line + sign * distance, which, other))
                    )
        return 0

    def take_cols(s):
        @pl.when(owns_cols)
        def _():
            cols[s] = full[s, pl.ds(aligned, span), :]

        @pl.when(jnp.logical_not(owns_cols))
        def _():
            pltpu.make_async_copy(cols.at[s], cols.at[s], col_recv.at[s]).wait()

    def multiply(d, k):
        row = pl.ds(pl.multiple_of(k * (rows // pieces), 16), rows // pieces)

        def one(n, _):
            sign = 1 - 2 * (n // 4)
            cross = lax.rem(n // 2, 2)
            distance = d - cross
            place = line + sign * distance
            good = jnp.logical_and(place >= 0, place < length)
            good = jnp.logical_and(good, distance >= n // 4)
            good = jnp.logical_and(good, distance >= 0)

            @pl.when(good)
            def _():
                s = index(place, lax.rem(side + cross, 2), lax.rem(n, 2))
                right = cols[s]
                if span != tile:
                    right = jnp.where(offset == aligned, right[:tile], right[span - tile:])
                product = lax.dot_general(
                    full[s, row, :], right, (((1,), (1,)), ((), ())), preferred_element_type=jnp.float32
                )
                for b in range(out_ref.shape[0]):
                    width = min(128, tile - b * 128)
                    out_ref[b, row, :width] += product[:, b * 128:b * 128 + width]

            return 0

        lax.fori_loop(0, 8, one, 0)

    def ready_own(k, _):
        s = index(line, side, 1 - core)
        arrived(s, k)
        to_peers(s, k)
        return 0

    lax.fori_loop(0, chunks, ready_own, 0)
    take_cols(me)
    take_cols(sibling)
    lax.fori_loop(1, length + 1, step, 0)

    def last(k, _):
        multiply(length, k)
        return 0

    lax.fori_loop(0, pieces, last, 0)

    def sent(s, way, first, count):
        ref = full.at[s, pl.ds(first * size, count * size)]
        pltpu.make_async_copy(ref, ref, send.at[way, s]).wait()

    def drain(place, _):
        straight, cross = index(place, side, core), index(place, 1 - side, core)
        sent(straight, 3, 0, chunks)
        sent(cross, 3, 0, chunks)
        pl.when(place == line)(lambda: sent(straight, 2, 0, chunks))
        pl.when(place != line)(lambda: sent(straight, 2, early, chunks - early))

        @pl.when(jnp.logical_and(has_up, place <= line))
        def _():
            sent(straight, 0, 0, chunks)
            sent(cross, 0, 0, early)

        @pl.when(jnp.logical_and(has_down, place >= line))
        def _():
            sent(straight, 1, 0, chunks)
            sent(cross, 1, 0, early)

        return 0

    lax.fori_loop(0, length, drain, 0)

    @pl.when(owns_cols)
    def _():
        for n in range(len(peers)):
            pltpu.make_async_copy(cols, cols, col_send.at[n]).wait()

    for n in range(len(peers)):
        pltpu.make_async_copy(sums.at[i], sums.at[i], sum_send.at[n]).wait()


def flatten(tile, group, gram_ref, flat_ref):
    many = gram_ref.shape[1] // group
    wide = group * tile // 128
    scale = jnp.float32(1.0 / (MEMBERS - 1))
    for s in range(wide):
        parts = []
        at = s * 128
        while at < (s + 1) * 128:
            r, c = at // tile, at % tile
            count = min(tile - c, (s + 1) * 128 - at)
            parts.append((r, c, count, at - s * 128))
            at += count
        lane = lax.broadcasted_iota(jnp.int32, (many, 128), 1)
        value = None
        for r, c, count, to in parts:
            shift = (to - c) % 128
            here = gram_ref[c // 128, pl.ds(r, many, stride=group), :]
            here = pltpu.roll(here, shift, 1) if shift else here
            if c % 128 + count > 128:
                then = gram_ref[c // 128 + 1, pl.ds(r, many, stride=group), :]
                then = pltpu.roll(then, shift, 1) if shift else then
                here = jnp.where(lane < to + 128 - c % 128, here, then)
            value = here if value is None else jnp.where(lane < to, value, here)
        flat_ref[pl.ds(s, many, stride=wide), :] = value * scale


def local(n_row, n_col, snapshots, area_weight):
    rows, depth = snapshots.shape
    tile = rows * n_row // n_col
    units = rows // 16
    chunks = max(n for n in range(1, MAX_CHUNKS + 1) if units % n == 0)
    pieces = max(n for n in range(1, 9) if units % n == 0)
    early = max(1, round(chunks / 6))
    span = tile + tile % 16
    blocks = -(-tile // 128)
    gram = pl.pallas_call(
        functools.partial(gather_gram, n_row, n_col, chunks, early, pieces, tile),
        out_shape=jax.ShapeDtypeStruct((blocks, rows, 128), jnp.float32),
        in_specs=[pl.BlockSpec(memory_space=pltpu.VMEM)] * 2,
        out_specs=pl.BlockSpec(memory_space=pltpu.VMEM),
        scratch_shapes=[
            pltpu.VMEM((n_col, rows, depth), jnp.bfloat16),
            pltpu.VMEM((n_col, span, depth), jnp.bfloat16),
            pltpu.VMEM((n_row, 8, depth), jnp.float32),
            pltpu.SemaphoreType.DMA((n_col, chunks)),
            pltpu.SemaphoreType.DMA((4, n_col)),
            pltpu.SemaphoreType.DMA((n_col,)),
            pltpu.SemaphoreType.DMA((max(n_row - 1, 1),)),
            pltpu.SemaphoreType.DMA((n_row,)),
            pltpu.SemaphoreType.DMA((max(n_row - 1, 1),)),
        ],
        compiler_params=pltpu.CompilerParams(
            collective_id=0, has_side_effects=True, vmem_limit_bytes=60 * 2**20
        ),
        name="gather_gram",
    )(snapshots, area_weight.reshape(1, depth))
    group = 8
    while group * tile % 128:
        group *= 2
    groups = rows // group
    block = 16 if groups % 16 == 0 else groups
    wide = group * tile // 128
    flat = pl.pallas_call(
        functools.partial(flatten, tile, group),
        grid=(groups // block,),
        out_shape=jax.ShapeDtypeStruct((groups * wide, 128), jnp.float32),
        in_specs=[pl.BlockSpec((blocks, block * group, 128), lambda n: (0, n, 0))],
        out_specs=pl.BlockSpec((block * wide, 128), lambda n: (n, 0)),
        name="flatten",
    )(gram)
    return flat.reshape(1, 1, rows * tile)


def solution(mesh):
    placed = (P("mrow", "pcol"), P("pcol"))
    return jax.shard_map(
        functools.partial(local, mesh.shape["mrow"], mesh.shape["pcol"]),
        mesh=mesh, in_specs=placed, out_specs=P("mrow", "pcol", None), check_vma=False,
    )
```

```python
import functools

import jax
import jax.numpy as jnp
from jax import lax
from jax.experimental import pallas as pl
from jax.experimental.pallas import tpu as pltpu
from jax.sharding import PartitionSpec as P

MEMBERS = 7424
MAX_CHUNKS = 8
MESH = pl.DeviceIdType.MESH


def gather_gram(
    n_row, n_col, chunks, early, pieces, tile, x_ref, weight_ref, out_ref, full, cols, sums, recv, send, col_recv, col_send,
    sum_recv, sum_send,
):
    rows, depth = x_ref.shape
    length = n_col // 4
    size = rows // chunks
    span = cols.shape[1]
    i = lax.axis_index("mrow")
    me = lax.axis_index("pcol")
    core = lax.rem(me, 2)
    side = lax.rem(me // 2, 2)
    line = me // 4
    ratio = n_col // n_row
    root = me // ratio
    offset = lax.rem(me, ratio) * tile
    aligned = pl.multiple_of(offset // 16 * 16, 16)
    my_chunk = (aligned + span - 1) // size
    stride = chunks // pieces

    def index(where, which, own):
        return (where * 2 + which) * 2 + own

    up, down = index(line + 1, side, core), index(line - 1, side, core)
    across, sibling = index(line, 1 - side, core), index(line, side, 1 - core)
    has_up, has_down = line + 1 < length, line >= 1
    peers = [lax.rem(i + step, n_row) for step in range(1, n_row)]
    owns_cols = root == i

    barrier = pltpu.get_barrier_semaphore()

    def greet(row, col):
        pl.semaphore_signal(barrier, inc=1, device_id=(row, col), device_id_type=MESH)

    pl.when(has_up)(lambda: greet(i, up))
    pl.when(has_down)(lambda: greet(i, down))
    greet(i, across)
    greet(i, sibling)
    for peer in peers:
        greet(peer, me)

    def add_up(k, total):
        block = x_ref[pl.ds(pl.multiple_of(k * size, 16), size), :].astype(jnp.float32)
        return total + jnp.sum(block.reshape(size // 8, 8, depth), axis=0)

    sums[i] = lax.fori_loop(0, chunks, add_up, jnp.zeros((8, depth), jnp.float32))
    pl.semaphore_wait(barrier, 2 + len(peers) + has_up.astype(jnp.int32) + has_down.astype(jnp.int32))

    def part(s, k):
        return full.at[s, pl.ds(pl.multiple_of(k * size, 16), size)]

    def copy(s, k, way, target):
        return pltpu.make_async_remote_copy(
            src_ref=part(s, k), dst_ref=part(s, k), send_sem=send.at[way, s], recv_sem=recv.at[s, k],
            device_id=(i, target), device_id_type=MESH,
        )

    def col_copy(s, n):
        return pltpu.make_async_remote_copy(
            src_ref=full.at[s, pl.ds(aligned, span)], dst_ref=cols.at[s], send_sem=col_send.at[n],
            recv_sem=col_recv.at[s], device_id=(peers[n], me), device_id_type=MESH,
        )

    def arrived(s, k):
        pltpu.make_async_copy(part(s, k), part(s, k), recv.at[s, k]).wait()

    def share(s, k):
        copy(s, k, 3, sibling).start()

    def to_peers(s, k):
        @pl.when(jnp.logical_and(owns_cols, k == my_chunk))
        def _():
            for n in range(len(peers)):
                col_copy(s, n).start()

    def go_up(s, k):
        pl.when(has_up)(lambda: copy(s, k, 0, up).start())

    def go_down(s, k):
        pl.when(has_down)(lambda: copy(s, k, 1, down).start())

    def sum_copy(n):
        return pltpu.make_async_remote_copy(
            src_ref=sums.at[i], dst_ref=sums.at[i], send_sem=sum_send.at[n], recv_sem=sum_recv.at[i],
            device_id=(peers[n], me), device_id_type=MESH,
        )

    for n in range(len(peers)):
        sum_copy(n).start()
    out_ref[...] = jnp.zeros_like(out_ref)
    for peer in peers:
        pltpu.make_async_copy(sums.at[peer], sums.at[peer], sum_recv.at[peer]).wait()
    mean = jnp.sum(jnp.sum(sums[...], axis=0), axis=0, keepdims=True) / MEMBERS
    root_weight = jnp.sqrt(weight_ref[...])

    def center(k):
        row = pl.ds(pl.multiple_of(k * size, 16), size)
        full[me, row, :] = ((x_ref[row, :].astype(jnp.float32) - mean) * root_weight).astype(jnp.bfloat16)

    def own(k, _):
        pl.when(k + 1 < chunks)(lambda: center(k + 1))
        copy(me, k, 2, across).start()
        go_up(me, k)
        go_down(me, k)
        share(me, k)
        to_peers(me, k)
        return 0

    center(0)
    lax.fori_loop(0, chunks, own, 0)

    def cross_first(k, _):
        arrived(across, k)
        go_up(across, k)
        go_down(across, k)
        share(across, k)
        to_peers(across, k)
        return 0

    lax.fori_loop(0, early, cross_first, 0)

    def valid(sign, distance):
        place = line + sign * distance
        inside = jnp.logical_and(place >= 0, place < length)
        far = distance >= 1 if sign > 0 else distance >= 0
        return jnp.logical_and(inside, far)

    def step(d, _):
        def from_sibling(k):
            for sign in (-1, 1):
                for which, distance in ((side, d), (1 - side, d - 1)):
                    @pl.when(valid(sign, distance))
                    def _():
                        s = index(line + sign * distance, which, 1 - core)
                        arrived(s, k)
                        to_peers(s, k)

        def piece(k, _):
            for sign, forward in ((-1, go_up), (1, go_down)):
                @pl.when(valid(sign, d))
                def _():
                    s = index(line + sign * d, side, core)
                    arrived(s, k)
                    forward(s, k)
                    pl.when(k >= early)(lambda: copy(s, k, 2, across).start())
                    share(s, k)
                    to_peers(s, k)

                    @pl.when(k < early)
                    def _():
                        t = index(line + sign * d, 1 - side, core)
                        arrived(t, k)
                        forward(t, k)
                        share(t, k)
                        to_peers(t, k)

            for sign in (-1, 1):
                @pl.when(jnp.logical_and(valid(sign, d - 1), k >= early))
                def _():
                    s = index(line + sign * (d - 1), 1 - side, core)
                    arrived(s, k)
                    share(s, k)
                    to_peers(s, k)

            pl.when(k >= 1)(lambda: from_sibling(k - 1))

            @pl.when(jnp.logical_and(lax.rem(k, stride) == stride - 1, k // stride < pieces))
            def _():
                multiply(d - 1, k // stride)

            return 0

        lax.fori_loop(0, chunks, piece, 0)
        from_sibling(chunks - 1)
        for sign in (-1, 1):
            for which, distance in ((side, d), (1 - side, d - 1)):
                for other in (core, 1 - core):
                    pl.when(valid(sign, distance))(
                        lambda: take_cols(index(line + sign * distance, which, other))
                    )
        return 0

    def take_cols(s):
        @pl.when(owns_cols)
        def _():
            cols[s] = full[s, pl.ds(aligned, span), :]

        @pl.when(jnp.logical_not(owns_cols))
        def _():
            pltpu.make_async_copy(cols.at[s], cols.at[s], col_recv.at[s]).wait()

    def multiply(d, k):
        row = pl.ds(pl.multiple_of(k * (rows // pieces), 16), rows // pieces)

        def one(n, _):
            sign = 1 - 2 * (n // 4)
            cross = lax.rem(n // 2, 2)
            distance = d - cross
            place = line + sign * distance
            good = jnp.logical_and(place >= 0, place < length)
            good = jnp.logical_and(good, distance >= n // 4)
            good = jnp.logical_and(good, distance >= 0)

            @pl.when(good)
            def _():
                s = index(place, lax.rem(side + cross, 2), lax.rem(n, 2))
                right = cols[s]
                if span != tile:
                    right = jnp.where(offset == aligned, right[:tile], right[span - tile:])
                product = lax.dot_general(
                    full[s, row, :], right, (((1,), (1,)), ((), ())), preferred_element_type=jnp.float32
                )
                for b in range(out_ref.shape[0]):
                    width = min(128, tile - b * 128)
                    out_ref[b, row, :width] += product[:, b * 128:b * 128 + width]

            return 0

        lax.fori_loop(0, 8, one, 0)

    def ready_own(k, _):
        s = index(line, side, 1 - core)
        arrived(s, k)
        to_peers(s, k)
        return 0

    lax.fori_loop(0, chunks, ready_own, 0)
    take_cols(me)
    take_cols(sibling)
    lax.fori_loop(1, length + 1, step, 0)

    def last(k, _):
        multiply(length, k)
        return 0

    lax.fori_loop(0, pieces, last, 0)

    def sent(s, way, first, count):
        ref = full.at[s, pl.ds(first * size, count * size)]
        pltpu.make_async_copy(ref, ref, send.at[way, s]).wait()

    def drain(place, _):
        straight, cross = index(place, side, core), index(place, 1 - side, core)
        sent(straight, 3, 0, chunks)
        sent(cross, 3, 0, chunks)
        pl.when(place == line)(lambda: sent(straight, 2, 0, chunks))
        pl.when(place != line)(lambda: sent(straight, 2, early, chunks - early))

        @pl.when(jnp.logical_and(has_up, place <= line))
        def _():
            sent(straight, 0, 0, chunks)
            sent(cross, 0, 0, early)

        @pl.when(jnp.logical_and(has_down, place >= line))
        def _():
            sent(straight, 1, 0, chunks)
            sent(cross, 1, 0, early)

        return 0

    lax.fori_loop(0, length, drain, 0)

    @pl.when(owns_cols)
    def _():
        for n in range(len(peers)):
            pltpu.make_async_copy(cols, cols, col_send.at[n]).wait()

    for n in range(len(peers)):
        pltpu.make_async_copy(sums.at[i], sums.at[i], sum_send.at[n]).wait()


def flatten(tile, group, gram_ref, flat_ref):
    many = gram_ref.shape[1] // group
    wide = group * tile // 128
    scale = jnp.float32(1.0 / (MEMBERS - 1))
    for s in range(wide):
        parts = []
        at = s * 128
        while at < (s + 1) * 128:
            r, c = at // tile, at % tile
            count = min(tile - c, (s + 1) * 128 - at)
            parts.append((r, c, count, at - s * 128))
            at += count
        lane = lax.broadcasted_iota(jnp.int32, (many, 128), 1)
        value = None
        for r, c, count, to in parts:
            shift = (to - c) % 128
            here = gram_ref[c // 128, pl.ds(r, many, stride=group), :]
            here = pltpu.roll(here, shift, 1) if shift else here
            if c % 128 + count > 128:
                then = gram_ref[c // 128 + 1, pl.ds(r, many, stride=group), :]
                then = pltpu.roll(then, shift, 1) if shift else then
                here = jnp.where(lane < to + 128 - c % 128, here, then)
            value = here if value is None else jnp.where(lane < to, value, here)
        flat_ref[pl.ds(s, many, stride=wide), :] = value * scale


def local(n_row, n_col, snapshots, area_weight):
    rows, depth = snapshots.shape
    tile = rows * n_row // n_col
    units = rows // 16
    chunks = max(n for n in range(1, MAX_CHUNKS + 1) if units % n == 0)
    pieces = max(n for n in range(1, 9) if units % n == 0)
    early = max(1, round(chunks / 6))
    span = tile + tile % 16
    blocks = -(-tile // 128)
    gram = pl.pallas_call(
        functools.partial(gather_gram, n_row, n_col, chunks, early, pieces, tile),
        out_shape=jax.ShapeDtypeStruct((blocks, rows, 128), jnp.float32),
        in_specs=[pl.BlockSpec(memory_space=pltpu.VMEM)] * 2,
        out_specs=pl.BlockSpec(memory_space=pltpu.VMEM),
        scratch_shapes=[
            pltpu.VMEM((n_col, rows, depth), jnp.bfloat16),
            pltpu.VMEM((n_col, span, depth), jnp.bfloat16),
            pltpu.VMEM((n_row, 8, depth), jnp.float32),
            pltpu.SemaphoreType.DMA((n_col, chunks)),
            pltpu.SemaphoreType.DMA((4, n_col)),
            pltpu.SemaphoreType.DMA((n_col,)),
            pltpu.SemaphoreType.DMA((max(n_row - 1, 1),)),
            pltpu.SemaphoreType.DMA((n_row,)),
            pltpu.SemaphoreType.DMA((max(n_row - 1, 1),)),
        ],
        compiler_params=pltpu.CompilerParams(
            collective_id=0, has_side_effects=True, vmem_limit_bytes=60 * 2**20
        ),
        name="gather_gram",
    )(snapshots, area_weight.reshape(1, depth))
    group = 8
    while group * tile % 128:
        group *= 2
    groups = rows // group
    block = max((n for n in range(8, 257, 8) if groups % n == 0), default=groups)
    wide = group * tile // 128
    flat = pl.pallas_call(
        functools.partial(flatten, tile, group),
        grid=(groups // block,),
        out_shape=jax.ShapeDtypeStruct((groups * wide, 128), jnp.float32),
        in_specs=[pl.BlockSpec((blocks, block * group, 128), lambda n: (0, n, 0))],
        out_specs=pl.BlockSpec((block * wide, 128), lambda n: (n, 0)),
        name="flatten",
    )(gram)
    return flat.reshape(1, 1, rows * tile)


def solution(mesh):
    placed = (P("mrow", "pcol"), P("pcol"))
    return jax.shard_map(
        functools.partial(local, mesh.shape["mrow"], mesh.shape["pcol"]),
        mesh=mesh, in_specs=placed, out_specs=P("mrow", "pcol", None), check_vma=False,
    )
```
